128 devices in a mesh: expert: 16 (over y, x_hi, core), dp: 8 (over x_lo, z).
Axes of the slice: x: 4 (x_hi: 2, x_lo: 2; x = x_hi * 2 + x_lo), y: 4, z: 4, core: 2. Of those that a mesh axis runs over, the one named last changes fastest.
Arguments:
- gradient: bfloat16 [8, 1, 14336, 2048], P('dp', None, None, 'expert'), may hold values from -6 to 6
- momentum: float32 [8, 1, 14336, 2048], P('dp', None, 'expert'), may hold values from -6 to 6
- group_index: int32 [224, 32, 8, 32], P('expert'), may hold values from 0 to 4095, all different within a row
Outputs:
- momentum_next: float32 [8, 1, 14336, 2048], P('dp', None, 'expert')
- update: float32 [1, 14336, 2048], P(None, None, 'expert')
The draws below stay inside these ranges and needn't reach their ends.
Inputs may be any that keep to these rules, and one draw needn't show every extreme that they name: `group_index`: an entry names the coefficient at row frequency (entry // 64) and column frequency (entry % 64) of its block; the 32 entries of one block and replica differ.
All inputs are finite; a program needn't handle non-finite values.
Results may differ from the reference program's by a relative error of at most 0.0003.
Values may be sent and summed in bfloat16 or wider, within the bound.
A program may use at most 192 MiB of HBM per device.

```python
import math
import jax
import jax.numpy as jnp
from jax import lax

D = 2048
FF = 14336
EXP = 1
SPAN = 64
TOPK = 32
REPL = 8
NCR = 224
NCC = 32
N_DP = 8


def block_scale(key, extent, split, low, largest):
    def one(dim, shards_of):
        heights = jax.random.uniform(jax.random.fold_in(jax.random.fold_in(key, 6), dim), (shards_of,), jnp.float32, low / len(split), largest / len(split))
        return jnp.repeat(jnp.exp(heights), extent[dim] // shards_of).reshape((-1,) + (1,) * (len(extent) - dim - 1))

    level = one(*split[0])
    for cut in split[1:]:
        level = level * one(*cut)
    return level


def choose_distinct(key, rows, number_of, top, lift):
    order = jax.random.permutation(jax.random.fold_in(key, 1), number_of)
    boost = order
    for power in range(3):
        boost = boost * boost // number_of
    boost = boost * lift // number_of
    chance = jax.random.randint(jax.random.fold_in(key, 2), (rows, number_of), 0, 4096) + boost
    fixed_rows = jax.random.permutation(jax.random.fold_in(key, 3), rows)[jnp.arange(number_of) % rows]
    chance = jnp.where(jnp.arange(rows)[:, None] == fixed_rows[None, :], 1 << 14, chance)
    merit = chance * number_of + jnp.arange(number_of)
    return lax.top_k(merit.astype(jnp.int32), top)[1].astype(jnp.int32)


def bell_draw(rng, dims, width, bound, cuts=(), kind=jnp.bfloat16):
    entries = jax.random.normal(rng, dims, jnp.float32) * width
    if len(cuts) > 0:
        entries = block_scale(rng, dims, cuts, -0.22, 0.18) * entries
    return jnp.clip(entries, min=-bound, max=bound).astype(kind)


def setup_inputs(seed: int = 0) -> dict:
    splits = jax.random.split(jax.random.key(seed), 4)
    return {
        "gradient": bell_draw(splits[0], (REPL, EXP, FF, D), 1.0, 6.0, ((0, 8), (3, 16))),
        "momentum": bell_draw(splits[1], (REPL, EXP, FF, D), 1.0, 6.0, ((0, 8), (2, 16)), jnp.float32),
        "group_index": choose_distinct(splits[2], NCR * NCC * REPL, SPAN * SPAN, TOPK, 0).reshape((NCR, NCC, REPL, TOPK)),
    }


MOMENTUM_DECAY = 0.999
HIGHEST_PRECISION = lax.Precision.HIGHEST

def cosine_table(order_size):
    frequency = jnp.arange(order_size, dtype=jnp.float32)[:, None]
    position = jnp.arange(order_size, dtype=jnp.float32)[None, :]
    weighting = jnp.where(frequency == 0, math.sqrt(1.0 / order_size), math.sqrt(2.0 / order_size))
    return weighting * jnp.cos(math.pi * (2.0 * position + 1.0) * frequency / (2.0 * order_size))

def reference(gradient, momentum, group_index):
    matrix = cosine_table(SPAN)
    block_rows = EXP * FF // SPAN
    block_cols = D // SPAN
    row_ids = jnp.arange(block_rows, dtype=jnp.int32)[:, None, None]
    col_ids = jnp.arange(block_cols, dtype=jnp.int32)[None, :, None]

    def one_replica(running, inputs):
        grad_part, mom_part, replica = inputs
        decayed = MOMENTUM_DECAY * mom_part + grad_part.astype(jnp.float32)
        blocks = decayed.reshape(block_rows, SPAN, block_cols, SPAN)
        coeffs = jnp.einsum('ui,piqj,vj->pquv', matrix, blocks, matrix, precision=HIGHEST_PRECISION)
        chosen = lax.dynamic_index_in_dim(group_index, replica, 2, keepdims=False)
        marked = jnp.zeros((block_rows, block_cols, SPAN * SPAN), jnp.float32).at[row_ids, col_ids, chosen].set(1.0)
        selected = coeffs * marked.reshape(block_rows, block_cols, SPAN, SPAN)
        restored = jnp.einsum('ui,pquv,vj->piqj', matrix, selected, matrix, precision=HIGHEST_PRECISION)
        return (running + restored.reshape(EXP, FF, D), (blocks - restored).reshape(EXP, FF, D))
    initial = jnp.zeros((EXP, FF, D), jnp.float32)
    replicas = jnp.arange(N_DP, dtype=jnp.int32)
    update, momentum_next = lax.scan(one_replica, initial, (gradient, momentum, replicas))
    return (momentum_next, update)
```

```python
import functools

import jax
import jax.numpy as jnp
import numpy as np
from jax import lax
from jax.experimental import pallas as pl
from jax.experimental.pallas import tpu as pltpu
from jax.sharding import PartitionSpec as P

SPAN = 64
TOPK = 32
DECAY = 0.999
LANES = 128
GROUP = 8

F32 = jnp.float32
BF16 = jnp.bfloat16


def cosine_table():
    u = np.arange(SPAN, dtype=np.float64)[:, None]
    i = np.arange(SPAN, dtype=np.float64)[None, :]
    weight = np.where(u == 0, np.sqrt(1.0 / SPAN), np.sqrt(2.0 / SPAN))
    return weight * np.cos(np.pi * (2.0 * i + 1.0) * u / (2.0 * SPAN))


def two_parts(x):
    high = x.astype(jnp.bfloat16.dtype)
    low = (x - high.astype(np.float64)).astype(jnp.bfloat16.dtype)
    return high, low


def tables():
    c = cosine_table()
    ct_high, ct_low = two_parts(c.T)
    ct = np.concatenate([ct_high, ct_low], axis=0)
    four = np.kron(np.eye(4), c)
    four_high, four_low = two_parts(four)
    return ct, np.stack([four_high, four_low])


def split(x):
    high = x.astype(BF16)
    return high, (x - high.astype(F32)).astype(BF16)


def dot(a, b):
    return jnp.dot(a, b, preferred_element_type=F32)


def dot_nt(a, b):
    return lax.dot_general(a, b, (((1,), (1,)), ((), ())), preferred_element_type=F32)


def values_of(x, picked, ct):
    rows = lax.broadcasted_iota(jnp.int32, (SPAN, LANES), 0)
    owner = lax.broadcasted_iota(jnp.int32, (SPAN, LANES), 1) // TOPK
    at_u = jnp.where(rows == (picked >> 6), 1.0, 0.0).astype(BF16)
    at_v = jnp.where(rows == (picked & 63), 1.0, 0.0).astype(BF16)
    both = dot(ct, jnp.concatenate([at_u, at_v], axis=1))
    left = both[:SPAN, :LANES] + both[SPAN:, :LANES]
    spread = []
    for part in (both[:SPAN, LANES:], both[SPAN:, LANES:]):
        spread.append(
            jnp.concatenate([jnp.where(owner == q, part, 0.0).astype(BF16) for q in range(4)], axis=0)
        )
    right = jnp.concatenate(spread, axis=1)
    if x.dtype == BF16:
        z = dot(x, right)
        z = z[:, :LANES] + z[:, LANES:]
    else:
        high, low = split(x)
        z = dot(jnp.concatenate([high, low], axis=0), right)
        z = z[:SPAN, :LANES] + (z[:SPAN, LANES:] + z[SPAN:, :LANES] + z[SPAN:, LANES:])
    return jnp.sum(left * z, axis=0, keepdims=True)


def inverse(s, ct, four_ref):
    high, low = split(s)
    z = dot(high, four_ref[0]) + (dot(low, four_ref[0]) + dot(high, four_ref[1]))
    high, low = split(z)
    y = dot(ct, high)
    return y[:SPAN] + (y[SPAN:] + dot(ct[:SPAN], low))


def values_wide_kernel(x_ref, picked_ref, ct_ref, out_ref):
    for n in range(GROUP):
        x = x_ref[:, n * 256 : (n + 1) * 256]
        out_ref[n : n + 1, :] = values_of(x, picked_ref[n : n + 1, :], ct_ref[...])


def values_tall_kernel(x_ref, picked_ref, ct_ref, out_ref):
    for n in range(GROUP):
        x = jnp.concatenate(
            [x_ref[n * 128 : n * 128 + SPAN, :], x_ref[n * 128 + SPAN : n * 128 + 128, :]], axis=1
        )
        out_ref[n : n + 1, :] = values_of(x, picked_ref[n : n + 1, :], ct_ref[...])


def remain_kernel(x_ref, picked_ref, value_ref, ct_ref, four_ref, out_ref):
    rows = lax.broadcasted_iota(jnp.int32, (SPAN, LANES), 0)
    rows4 = lax.broadcasted_iota(jnp.int32, (256, LANES), 0)
    owner = lax.broadcasted_iota(jnp.int32, (1, LANES), 1) // TOPK
    for n in range(GROUP):
        picked = picked_ref[n : n + 1, :]
        value = value_ref[n : n + 1, :]
        high = value.astype(BF16).astype(F32)
        at_u = rows == (picked >> 6)
        left = jnp.concatenate(
            [jnp.where(at_u, high, 0.0).astype(BF16), jnp.where(at_u, value - high, 0.0).astype(BF16)],
            axis=0,
        )
        at_v = jnp.where(rows4 == (owner * SPAN + (picked & 63)), 1.0, 0.0).astype(BF16)
        s = dot_nt(left, at_v)
        restored = inverse(s[:SPAN] + s[SPAN:], ct_ref[...], four_ref)
        here = slice(n * 256, (n + 1) * 256)
        out_ref[:, here] = DECAY * x_ref[:, here] - restored


def update_kernel(picked_ref, value_ref, ct_ref, four_ref, out_ref, s_ref):
    rows = lax.broadcasted_iota(jnp.int32, (SPAN, 256), 0)
    for n in range(GROUP):
        for b in range(4):
            k = n * 4 + b
            picked = picked_ref[k : k + 1, :]
            value = value_ref[k : k + 1, :]
            high = value.astype(BF16).astype(F32)
            at_u = rows == (picked >> 6)
            left = jnp.concatenate(
                [
                    jnp.where(at_u, high, 0.0).astype(BF16),
                    jnp.where(at_u, value - high, 0.0).astype(BF16),
                ],
                axis=0,
            )
            at_v = jnp.where(rows == (picked & 63), 1.0, 0.0).astype(BF16)
            s = dot_nt(left, at_v)
            s_ref[n, :, b * SPAN : (b + 1) * SPAN] = s[:SPAN] + s[SPAN:]
        restored = inverse(s_ref[n], ct_ref[...], four_ref)
        out_ref[n * 128 : n * 128 + SPAN, :] = restored[:, :LANES]
        out_ref[n * 128 + SPAN : n * 128 + 128, :] = restored[:, LANES:]


def whole(shape):
    return pl.BlockSpec(shape, lambda i: (0,) * len(shape))


def params():
    return pltpu.CompilerParams(dimension_semantics=("arbitrary",))


def values_wide(x, picked, ct):
    rows, cols = x.shape
    return pl.pallas_call(
        values_wide_kernel,
        grid=(rows // SPAN,),
        in_specs=[
            pl.BlockSpec((SPAN, cols), lambda i: (i, 0)),
            pl.BlockSpec((GROUP, LANES), lambda i: (i, 0)),
            whole(ct.shape),
        ],
        out_specs=pl.BlockSpec((GROUP, LANES), lambda i: (i, 0)),
        out_shape=jax.ShapeDtypeStruct(picked.shape, F32),
        compiler_params=params(),
        name="values_wide",
    )(x, picked, ct)


def values_tall(x, picked, ct):
    rows, cols = x.shape
    return pl.pallas_call(
        values_tall_kernel,
        grid=(rows // (GROUP * 128),),
        in_specs=[
            pl.BlockSpec((GROUP * 128, cols), lambda i: (i, 0)),
            pl.BlockSpec((GROUP, LANES), lambda i: (i, 0)),
            whole(ct.shape),
        ],
        out_specs=pl.BlockSpec((GROUP, LANES), lambda i: (i, 0)),
        out_shape=jax.ShapeDtypeStruct(picked.shape, F32),
        compiler_params=params(),
        name="values_tall",
    )(x, picked, ct)


def remain(x, picked, value, ct, four):
    rows, cols = x.shape
    return pl.pallas_call(
        remain_kernel,
        grid=(rows // SPAN,),
        in_specs=[
            pl.BlockSpec((SPAN, cols), lambda i: (i, 0)),
            pl.BlockSpec((GROUP, LANES), lambda i: (i, 0)),
            pl.BlockSpec((GROUP, LANES), lambda i: (i, 0)),
            whole(ct.shape),
            whole(four.shape),
        ],
        out_specs=pl.BlockSpec((SPAN, cols), lambda i: (i, 0)),
        out_shape=jax.ShapeDtypeStruct(x.shape, F32),
        compiler_params=params(),
        name="remain",
    )(x, picked, value, ct, four)


def update_of(picked, value, rows, ct, four):
    blocks = picked.shape[0]
    step = GROUP * 4
    return pl.pallas_call(
        update_kernel,
        grid=(blocks // step,),
        in_specs=[
            pl.BlockSpec((step, 256), lambda i: (i, 0)),
            pl.BlockSpec((step, 256), lambda i: (i, 0)),
            whole(ct.shape),
            whole(four.shape),
        ],
        out_specs=pl.BlockSpec((GROUP * 128, LANES), lambda i: (i, 0)),
        out_shape=jax.ShapeDtypeStruct((rows, LANES), F32),
        scratch_shapes=[pltpu.VMEM((GROUP, SPAN, 256), F32)],
        compiler_params=params(),
        name="update",
    )(picked, value, ct, four)


def finish(left, arrived):
    def kernel(a_ref, g_ref, out_ref):
        for e in range(g_ref.shape[0]):
            here = slice(e * LANES, (e + 1) * LANES)
            out_ref[:, here] = a_ref[:, here] + g_ref[e].astype(F32)

    rows, cols = left.shape
    tall = 64
    return pl.pallas_call(
        kernel,
        grid=(rows // tall,),
        in_specs=[
            pl.BlockSpec((tall, cols), lambda i: (i, 0)),
            pl.BlockSpec((arrived.shape[0], tall, LANES), lambda i: (0, i, 0)),
        ],
        out_specs=pl.BlockSpec((tall, cols), lambda i: (i, 0)),
        out_shape=jax.ShapeDtypeStruct(left.shape, F32),
        compiler_params=params(),
        name="finish",
    )(left, arrived)


def on_device(gradient, momentum, group_index):
    ct, four = (jnp.asarray(t) for t in tables())
    ways = lax.axis_size("expert")
    replicas = lax.axis_size("dp")
    replica = lax.axis_index("dp")
    total_rows = gradient.shape[2]
    rows, cols = momentum.shape[2:]
    block_rows, block_cols = rows // SPAN, cols // SPAN
    wide = block_cols // ways

    gradient = gradient.reshape(total_rows, LANES)
    momentum = momentum.reshape(rows, cols)

    parts = group_index.reshape(block_rows, ways, wide, replicas, TOPK).transpose(1, 0, 2, 3, 4)
    columns = lax.all_to_all(parts, "expert", 0, 0, tiled=True)
    columns = columns.reshape(ways * block_rows * wide, replicas, TOPK)
    own_rows = lax.dynamic_index_in_dim(group_index, replica, 2, keepdims=False).reshape(-1, LANES)
    own_cols = lax.dynamic_index_in_dim(columns, replica, 1, keepdims=False).reshape(-1, LANES)

    arrived = lax.all_to_all(gradient.reshape(ways, rows, LANES), "expert", 0, 0, tiled=True)

    from_rows = DECAY * values_wide(momentum, own_rows, ct)
    from_cols = values_tall(gradient, own_cols, ct)
    out_rows = (
        from_rows.reshape(block_rows, ways, wide * TOPK).transpose(1, 0, 2).reshape(ways, 1, -1)
    )
    out_cols = from_cols.reshape(ways, 1, block_rows * wide * TOPK)
    swapped = lax.all_to_all(jnp.concatenate([out_rows, out_cols], axis=1), "expert", 0, 0, tiled=True)
    at_cols = swapped[:, 0].reshape(-1) + from_cols.reshape(-1)
    back = swapped[:, 1].reshape(ways, block_rows, wide * TOPK).transpose(1, 0, 2)
    at_rows = back.reshape(-1, LANES) + from_rows

    everyone = lax.all_gather(at_cols.reshape(-1, TOPK), "dp", axis=1, tiled=False)
    update = update_of(columns.reshape(-1, 256), everyone.reshape(-1, 256), total_rows, ct, four)
    left = remain(momentum, own_rows, at_rows, ct, four)
    momentum_next = finish(left, arrived)
    return momentum_next.reshape(1, 1, rows, cols), update.reshape(1, total_rows, LANES)


def solution(mesh):
    return jax.shard_map(
        on_device,
        mesh=mesh,
        in_specs=(
            P("dp", None, None, "expert"),
            P("dp", None, "expert", None),
            P("expert", None, None, None),
        ),
        out_specs=(P("dp", None, "expert", None), P(None, None, "expert")),
        check_vma=False,
    )
```

```python
import functools

import jax
import jax.numpy as jnp
import numpy as np
from jax import lax
from jax.experimental import pallas as pl
from jax.experimental.pallas import tpu as pltpu
from jax.sharding import PartitionSpec as P

SPAN = 64
TOPK = 32
DECAY = 0.999
LANES = 128
EARLY = 192
IN_KERNEL = 896

F32 = jnp.float32
BF16 = jnp.bfloat16
MESH = pl.DeviceIdType.MESH
ANY = pl.BlockSpec(memory_space=pl.ANY)
VMEM = pl.BlockSpec(memory_space=pltpu.VMEM)


def cosine_table():
    u = np.arange(SPAN, dtype=np.float64)[:, None]
    i = np.arange(SPAN, dtype=np.float64)[None, :]
    weight = np.where(u == 0, np.sqrt(1.0 / SPAN), np.sqrt(2.0 / SPAN))
    return weight * np.cos(np.pi * (2.0 * i + 1.0) * u / (2.0 * SPAN))


def two_parts(x):
    high = x.astype(jnp.bfloat16.dtype)
    low = (x - high.astype(np.float64)).astype(jnp.bfloat16.dtype)
    return high, low


def tables():
    c = cosine_table()
    turned = np.zeros((SPAN, LANES), np.float32)
    turned[:, :SPAN] = c.T
    owner = np.arange(LANES)[None, None, :] // TOPK == np.arange(4)[:, None, None]
    owner = np.broadcast_to(owner, (4, SPAN, LANES)).astype(jnp.bfloat16.dtype)
    return turned, owner, np.stack(two_parts(np.kron(np.eye(4), c)))


def split(x):
    high = x.astype(BF16)
    return high, (x - high.astype(F32)).astype(BF16)


def dot(a, b):
    return jnp.dot(a, b, preferred_element_type=F32)


def dot_nt(a, b):
    return lax.dot_general(a, b, (((1,), (1,)), ((), ())), preferred_element_type=F32)


def columns_of(table, row):
    where = jnp.broadcast_to(row, table.shape)
    return jnp.take_along_axis(table, where, axis=1, mode="promise_in_bounds")


def spread(part, owner_ref):
    return jnp.concatenate([part * owner_ref[q] for q in range(4)], axis=0)


def right_side(picked, turned, owner_ref):
    high, low = split(columns_of(turned, picked & 63))
    return jnp.concatenate([spread(high, owner_ref), spread(low, owner_ref)], axis=1)


def values_of(x, picked, turned, owner_ref):
    right = right_side(picked, turned, owner_ref)
    if x.dtype == BF16:
        z = dot(x, right)
        z = z[:, :LANES] + z[:, LANES:]
    else:
        z = dot(jnp.concatenate(split(x), axis=0), right)
        z = z[:SPAN, :LANES] + (z[:SPAN, LANES:] + z[SPAN:, :LANES] + z[SPAN:, LANES:])
    return jnp.sum(columns_of(turned, picked >> 6) * z, axis=0, keepdims=True)


def restored_of(picked, value, turned, owner_ref):
    high, low = split(columns_of(turned, picked >> 6) * value)
    left = jnp.concatenate(
        [jnp.concatenate([high, high], axis=1), jnp.concatenate([low, low], axis=1)], axis=0
    )
    r = dot_nt(left, right_side(picked, turned, owner_ref))
    return r[:SPAN] + r[SPAN:]


def pair(ref, j):
    top = ref[j * 128 : j * 128 + SPAN, :]
    return jnp.concatenate([top, ref[j * 128 + SPAN : (j + 1) * 128, :]], axis=1)


def exchange_kernel(
    gradient, momentum, picked, turned, owner,
    left, all_picked, all_value, arrived,
    mbuf, gbuf, col_picked, row_value, row_in, col_value, col_in, total,
    msem, gsem, lsem, osem, isend, irecv, rsend, rrecv, csend, crecv, asend, arecv, bsend, brecv,
    psend, precv,
    *, ways, replicas, early, rows_here,
):
    e = lax.axis_index("expert")
    r = lax.axis_index("dp")
    rows = mbuf.shape[1]
    units = rows // 128

    barrier = pltpu.get_barrier_semaphore()
    for d in range(1, ways):
        pl.semaphore_signal(barrier, inc=1, device_id={"expert": e ^ d}, device_id_type=MESH)
    for d in range(1, replicas):
        pl.semaphore_signal(barrier, inc=1, device_id={"dp": r ^ d}, device_id_type=MESH)

    def fetch_m(s):
        columns = pl.ds(pl.multiple_of(s * LANES, LANES), LANES)
        return pltpu.make_async_copy(momentum.at[:, columns], mbuf.at[s], msem.at[s])

    def fetch_g(s):
        here = pl.ds(pl.multiple_of(s * rows, 128), rows)
        return pltpu.make_async_copy(gradient.at[here], gbuf.at[s], gsem.at[s])

    @pl.loop(0, ways)
    def _(s):
        fetch_m(s).start()

    @pl.loop(0, ways)
    def _(s):
        fetch_g(s).start()

    pl.semaphore_wait(barrier, ways - 1 + replicas - 1)

    def to_expert(src, dst, send, recv, d):
        return pltpu.make_async_remote_copy(
            src_ref=src.at[e ^ d],
            dst_ref=dst.at[e],
            send_sem=send.at[d],
            recv_sem=recv.at[d],
            device_id={"expert": e ^ d},
            device_id_type=MESH,
        )

    def to_replica(src, dst, send, recv, d):
        return pltpu.make_async_remote_copy(
            src_ref=src,
            dst_ref=dst.at[r],
            send_sem=send.at[d],
            recv_sem=recv.at[d],
            device_id={"dp": r ^ d},
            device_id_type=MESH,
        )

    def bulk(d, part):
        start, size = ((0, early), (early, rows_here - early))[part]
        source = pl.ds(pl.multiple_of((e ^ d) * rows + start, 16), size)
        return pltpu.make_async_remote_copy(
            src_ref=gradient.at[source],
            dst_ref=arrived.at[e, pl.ds(start, size)],
            send_sem=bsend.at[part, d],
            recv_sem=brecv.at[part, d],
            device_id={"expert": e ^ d},
            device_id_type=MESH,
        )

    order = [d for d in range(1, ways) if d & 2] + [d for d in range(1, ways) if not d & 2]

    indices = [to_expert(picked, col_picked, isend, irecv, d) for d in order]
    for copy in indices:
        copy.start()
    first = [bulk(d, 0) for d in order]
    for copy in first:
        copy.start()
    col_picked[e] = picked[e]

    zero = jnp.zeros((1, LANES), F32)

    def values(out, source, where, fetch):
        @pl.loop(0, ways)
        def _(s):
            fetch(s).wait()
            found = [
                values_of(pair(source.at[s], j), where[s, j : j + 1, :], turned[...], owner)
                for j in range(units)
            ]
            out[s] = jnp.concatenate(found + [zero] * (8 - units), axis=0)

    values(row_value, mbuf, picked, fetch_m)
    rows_out = [to_expert(row_value, row_in, rsend, rrecv, d) for d in order]
    for copy in rows_out:
        copy.start()
    row_in[e] = row_value[e]

    for copy in indices:
        copy.wait()
    picked_out = [to_replica(col_picked, all_picked, asend, arecv, d) for d in range(1, replicas)]
    for copy in picked_out:
        copy.start()
    all_picked[r] = col_picked[...]

    values(col_value, gbuf, col_picked, fetch_g)
    cols_out = [to_expert(col_value, col_in, csend, crecv, d) for d in order]
    for copy in cols_out:
        copy.start()
    col_in[e] = col_value[e]

    for copy in rows_out:
        copy.wait()
    total[...] = DECAY * row_in[...] + col_value[...]
    value_out = [to_replica(total, all_value, psend, precv, d) for d in range(1, replicas)]
    for copy in value_out:
        copy.start()
    all_value[r] = total[...]

    own_slab = pltpu.make_async_copy(
        gbuf.at[e, pl.ds(0, rows_here)], arrived.at[e], lsem
    )
    own_slab.start()

    for copy in cols_out:
        copy.wait()
    second = [bulk(d, 1) for d in order] if rows_here > early else []
    for copy in second:
        copy.start()

    def back(s):
        return pltpu.make_async_copy(mbuf.at[s], left.at[s], osem.at[s])

    @pl.loop(0, ways)
    def _(s):
        value = DECAY * row_value[s] + col_in[s]
        for j in range(units):
            restored = restored_of(
                picked[s, j : j + 1, :], value[j : j + 1, :], turned[...], owner
            )
            for h in range(2):
                here = slice(j * 128 + h * SPAN, j * 128 + (h + 1) * SPAN)
                mbuf[s, here, :] = DECAY * mbuf[s, here, :] - restored[:, h * LANES : (h + 1) * LANES]
        back(s).start()

    @pl.loop(0, ways)
    def _(s):
        back(s).wait()

    own_slab.wait()
    for copy in picked_out + value_out + first + second:
        copy.wait()


def exchange(gradient, momentum, picked, turned, owner, ways, replicas):
    rows = momentum.shape[0]
    tile = (ways, 8, LANES)
    dma = pltpu.SemaphoreType.DMA
    return pl.pallas_call(
        functools.partial(
            exchange_kernel, ways=ways, replicas=replicas, early=EARLY, rows_here=IN_KERNEL
        ),
        in_specs=[ANY, ANY, VMEM, VMEM, VMEM],
        out_specs=[ANY, VMEM, VMEM, ANY],
        out_shape=[
            jax.ShapeDtypeStruct((ways, rows, LANES), F32),
            jax.ShapeDtypeStruct((replicas, *tile), jnp.int32),
            jax.ShapeDtypeStruct((replicas, *tile), F32),
            jax.ShapeDtypeStruct((ways, IN_KERNEL, LANES), BF16),
        ],
        scratch_shapes=[
            pltpu.VMEM((ways, rows, LANES), F32),
            pltpu.VMEM((ways, rows, LANES), BF16),
            pltpu.VMEM(tile, jnp.int32),
            *[pltpu.VMEM(tile, F32)] * 5,
            dma((ways,)),
            dma((ways,)),
            dma,
            dma((ways,)),
            *[dma((ways,))] * 6,
            *[dma((replicas,))] * 2,
            *[dma((2, ways))] * 2,
            *[dma((replicas,))] * 2,
        ],
        compiler_params=pltpu.CompilerParams(
            collective_id=0, has_side_effects=True, vmem_limit_bytes=24 << 20
        ),
        name="exchange",
    )(gradient, momentum, picked, turned, owner)


def update_kernel(picked_ref, value_ref, turned_ref, four_ref, out_hbm, th_ref, tl_ref, obuf, osem, *, units):
    steps = picked_ref.shape[0] // (4 * units)
    tall = units * 128
    rows = lax.broadcasted_iota(jnp.int32, (SPAN, 256), 0)

    def back(s):
        here = pl.ds(pl.multiple_of(s * tall, 128), tall)
        return pltpu.make_async_copy(obuf.at[here], out_hbm.at[here], osem.at[s])

    @pl.loop(0, steps)
    def _(s):
        for n in range(units):
            parts = []
            for b in range(4):
                k = (s * units + n) * 4 + b
                picked = picked_ref[pl.ds(k, 1), :]
                value = value_ref[pl.ds(k, 1), :]
                u = picked >> 6
                w = [columns_of(turned_ref[...], u[:, h * LANES : (h + 1) * LANES]) for h in range(2)]
                w = jnp.concatenate(w, axis=1) * value
                at_v = jnp.where(rows == (picked & 63), 1.0, 0.0).astype(BF16)
                t = dot_nt(jnp.concatenate(split(w), axis=0), at_v)
                parts.append(t[:SPAN] + t[SPAN:])
            high, low = split(jnp.concatenate(parts, axis=1))
            th_ref[n * SPAN : (n + 1) * SPAN, :] = high
            tl_ref[n * SPAN : (n + 1) * SPAN, :] = low
        r = dot(th_ref[...], four_ref[0]) + (dot(tl_ref[...], four_ref[0]) + dot(th_ref[...], four_ref[1]))
        for n in range(units):
            for h in range(2):
                here = pl.ds(pl.multiple_of(s * tall + n * 128 + h * SPAN, SPAN), SPAN)
                obuf[here, :] = r[n * SPAN : (n + 1) * SPAN, h * LANES : (h + 1) * LANES]
        back(s).start()

    @pl.loop(0, steps)
    def _(s):
        back(s).wait()


def update_of(picked, value, turned, four, units=8):
    blocks = picked.shape[0]
    rows = blocks * 32
    buf = pltpu.VMEM((units * SPAN, 256), BF16)
    return pl.pallas_call(
        functools.partial(update_kernel, units=units),
        in_specs=[VMEM] * 4,
        out_specs=ANY,
        out_shape=jax.ShapeDtypeStruct((rows, LANES), F32),
        scratch_shapes=[
            buf,
            buf,
            pltpu.VMEM((rows, LANES), F32),
            pltpu.SemaphoreType.DMA((blocks // (4 * units),)),
        ],
        compiler_params=pltpu.CompilerParams(vmem_limit_bytes=16 << 20),
        cost_estimate=pl.CostEstimate(flops=16_000_000_000, bytes_accessed=8_000_000, transcendentals=0),
        name="update",
    )(picked, value, turned, four)


def finish_kernel(left, *refs, starts):
    parts = len(starts)
    arrived, out, lbuf, gbuf, lsem, gsem, osem = refs[:parts], *refs[parts:]
    ways, rows = lbuf.shape[:2]

    def fetch(s):
        copies = [pltpu.make_async_copy(left.at[s], lbuf.at[s], lsem.at[s])]
        for n, (start, ref) in enumerate(zip(starts, arrived)):
            here = gbuf.at[s, pl.ds(start, ref.shape[1])]
            copies.append(pltpu.make_async_copy(ref.at[s], here, gsem.at[n, s]))
        return copies

    def back(s):
        columns = pl.ds(pl.multiple_of(s * LANES, LANES), LANES)
        return pltpu.make_async_copy(lbuf.at[s], out.at[:, columns], osem.at[s])

    @pl.loop(0, ways)
    def _(s):
        for copy in fetch(s):
            copy.start()

    @pl.loop(0, ways)
    def _(s):
        for copy in fetch(s):
            copy.wait()
        lbuf[s] = lbuf[s] + gbuf[s].astype(F32)
        back(s).start()

    @pl.loop(0, ways)
    def _(s):
        back(s).wait()


def finish(left, arrived):
    ways, rows, _ = left.shape
    starts = [sum(a.shape[1] for a in arrived[:n]) for n in range(len(arrived))]
    dma = pltpu.SemaphoreType.DMA
    return pl.pallas_call(
        functools.partial(finish_kernel, starts=tuple(starts)),
        in_specs=[ANY] * (1 + len(arrived)),
        out_specs=ANY,
        out_shape=jax.ShapeDtypeStruct((rows, ways * LANES), F32),
        scratch_shapes=[
            pltpu.VMEM(left.shape, F32),
            pltpu.VMEM(left.shape, BF16),
            dma((ways,)),
            dma((len(arrived), ways)),
            dma((ways,)),
        ],
        compiler_params=pltpu.CompilerParams(vmem_limit_bytes=16 << 20),
        name="finish",
    )(left, *arrived)


def on_device(gradient, momentum, group_index):
    turned, owner, four = (jnp.asarray(t) for t in tables())
    ways = lax.axis_size("expert")
    replicas = lax.axis_size("dp")
    total_rows = gradient.shape[2]
    rows, cols = momentum.shape[2:]
    units = rows // 128
    wide = cols // SPAN // ways

    gradient = gradient.reshape(total_rows, LANES)
    momentum = momentum.reshape(rows, cols)

    own = lax.dynamic_index_in_dim(group_index, lax.axis_index("dp"), 2, keepdims=False)
    own = own.reshape(units, 2, ways, wide, TOPK).transpose(2, 0, 1, 3, 4).reshape(ways, units, LANES)
    own = jnp.pad(own, ((0, 0), (0, 8 - units), (0, 0)))

    left, all_picked, all_value, arrived = exchange(
        gradient, momentum, own, turned, owner, ways, replicas
    )

    def by_block(x):
        x = x[:, :, :units].reshape(replicas, ways * units * 4, TOPK)
        return x.transpose(1, 0, 2).reshape(ways * units * 4, replicas * TOPK)

    pieces = [arrived]
    if IN_KERNEL < rows:
        gradient, all_value = lax.optimization_barrier((gradient, all_value))
        rest = gradient.reshape(ways, rows, LANES)[:, IN_KERNEL:]
        pieces.append(lax.all_to_all(rest, "expert", 0, 0, tiled=True))
    update = update_of(by_block(all_picked), by_block(all_value), turned, four)
    momentum_next = finish(left, pieces)
    return momentum_next.reshape(1, 1, rows, cols), update.reshape(1, total_rows, LANES)


def solution(mesh):
    return jax.shard_map(
        on_device,
        mesh=mesh,
        in_specs=(
            P("dp", None, None, "expert"),
            P("dp", None, "expert", None),
            P("expert", None, None, None),
        ),
        out_specs=(P("dp", None, "expert", None), P(None, None, "expert")),
        check_vma=False,
    )
```

```python
import functools

import jax
import jax.numpy as jnp
import numpy as np
from jax import lax
from jax.experimental import pallas as pl
from jax.experimental.pallas import tpu as pltpu
from jax.sharding import PartitionSpec as P

SPAN = 64
TOPK = 32
DECAY = 0.999
LANES = 128
CUTS = (0, 192, 320, 896)

F32 = jnp.float32
BF16 = jnp.bfloat16
MESH = pl.DeviceIdType.MESH
VMEM = pl.BlockSpec(memory_space=pltpu.VMEM)


def cosine_table():
    u = np.arange(SPAN, dtype=np.float64)[:, None]
    i = np.arange(SPAN, dtype=np.float64)[None, :]
    weight = np.where(u == 0, np.sqrt(1.0 / SPAN), np.sqrt(2.0 / SPAN))
    return weight * np.cos(np.pi * (2.0 * i + 1.0) * u / (2.0 * SPAN))


def two_parts(x):
    high = x.astype(jnp.bfloat16.dtype)
    low = (x - high.astype(np.float64)).astype(jnp.bfloat16.dtype)
    return high, low


def tables():
    c = cosine_table()
    turned = np.zeros((SPAN, LANES), np.float32)
    turned[:, :SPAN] = c.T
    return turned, np.stack(two_parts(np.kron(np.eye(4), c)))


def split(x):
    high = x.astype(BF16)
    return high, (x - high.astype(F32)).astype(BF16)


def dot(a, b):
    return jnp.dot(a, b, preferred_element_type=F32)


def dot_nt(a, b):
    return lax.dot_general(a, b, (((1,), (1,)), ((), ())), preferred_element_type=F32)


def columns_of(table, row):
    where = jnp.broadcast_to(row, table.shape)
    return jnp.take_along_axis(table, where, axis=1, mode="promise_in_bounds")


def spread(part, owner_ref):
    return jnp.concatenate([part * owner_ref[q] for q in range(4)], axis=0)


def right_side(picked, turned, owner_ref):
    high, low = split(columns_of(turned, picked & 63))
    return jnp.concatenate([spread(high, owner_ref), spread(low, owner_ref)], axis=1)


def values_of(x, picked, turned, owner_ref):
    right = right_side(picked, turned, owner_ref)
    if x.dtype == BF16:
        z = dot(x, right)
        z = z[:, :LANES] + z[:, LANES:]
    else:
        z = dot(jnp.concatenate(split(x), axis=0), right)
        z = z[:SPAN, :LANES] + (z[:SPAN, LANES:] + z[SPAN:, :LANES] + z[SPAN:, LANES:])
    return jnp.sum(columns_of(turned, picked >> 6) * z, axis=0, keepdims=True)


def restored_of(picked, value, turned, owner_ref):
    high, low = split(columns_of(turned, picked >> 6) * value)
    left = jnp.concatenate(
        [jnp.concatenate([high, high], axis=1), jnp.concatenate([low, low], axis=1)], axis=0
    )
    r = dot_nt(left, right_side(picked, turned, owner_ref))
    return r[:SPAN] + r[SPAN:]


def block_rows_of(found):
    replica = lax.broadcasted_iota(jnp.int32, (8, LANES), 0)
    group = lax.broadcasted_iota(jnp.int32, (8, LANES), 1) >> 5
    turned = found
    for n in range(1, 4):
        turned = jnp.where((replica & 3) == n, pltpu.roll(found, TOPK * n, 1), turned)
    rows = []
    for b in range(4):
        here = turned if b == 0 else pltpu.roll(turned, LANES - TOPK * b, 1)
        here = jnp.where((replica & 3) == group, here, jnp.zeros_like(here))
        here = here + pltpu.roll(here, 1, 0)
        here = here + pltpu.roll(here, 2, 0)
        rows.append((here[3:4], here[7:8]))
    return rows


def step_kernel(
    gradient, momentum, picked, turned_hbm, four_hbm,
    mn, update,
    gbuf, arrived, turned, owner, four, col_picked, row_value, row_in, col_value, col_in,
    all_picked, all_value, th, tl,
    msem, gsem, csem, isend, irecv, rsend, rrecv, csend, crecv, bsend, brecv,
    asend, arecv, psend, precv,
    *, ways, replicas, cuts,
):
    e = lax.axis_index("expert")
    r = lax.axis_index("dp")
    rows = gbuf.shape[1]
    units = rows // 128
    tiles = ways * 8

    barrier = pltpu.get_barrier_semaphore()
    for d in range(1, ways):
        pl.semaphore_signal(barrier, inc=1, device_id={"expert": e ^ d}, device_id_type=MESH)
    near = (1, 2, 3, 4)
    for d in near:
        pl.semaphore_signal(barrier, inc=1, device_id={"dp": r ^ d}, device_id_type=MESH)

    def columns(s):
        return pl.ds(pl.multiple_of(s * LANES, LANES), LANES)

    def fetch_m(s):
        return pltpu.make_async_copy(momentum.at[:, columns(s)], mn.at[:, columns(s)], msem.at[s])

    def fetch_g(s):
        here = pl.ds(pl.multiple_of(s * rows, 128), rows)
        return pltpu.make_async_copy(gradient.at[here], gbuf.at[s], gsem.at[s])

    constants = [
        pltpu.make_async_copy(turned_hbm, turned, csem.at[0]),
        pltpu.make_async_copy(four_hbm, four, csem.at[1]),
    ]
    constants[0].start()

    @pl.loop(0, ways)
    def _(s):
        fetch_m(s).start()

    @pl.loop(0, ways)
    def _(s):
        fetch_g(s).start()

    constants[1].start()
    lanes = lax.broadcasted_iota(jnp.int32, (SPAN, LANES), 1) >> 5
    for q in range(4):
        owner[q] = jnp.where(lanes == q, 1.0, 0.0).astype(BF16)

    pl.semaphore_wait(barrier, ways - 1 + len(near))

    def to_expert(src, dst, send, recv, d):
        return pltpu.make_async_remote_copy(
            src_ref=src.at[e ^ d],
            dst_ref=dst.at[e],
            send_sem=send.at[d],
            recv_sem=recv.at[d],
            device_id={"expert": e ^ d},
            device_id_type=MESH,
        )

    def to_replica(buf, slot, send, recv, d, n):
        here = pl.ds(pl.multiple_of(slot * tiles, 8), tiles)
        return pltpu.make_async_remote_copy(
            src_ref=buf.at[here],
            dst_ref=buf.at[here],
            send_sem=send.at[n],
            recv_sem=recv.at[n],
            device_id={"dp": r ^ d},
            device_id_type=MESH,
        )

    def bulk(d, part):
        start, size = cuts[part], cuts[part + 1] - cuts[part]
        source = pl.ds(pl.multiple_of((e ^ d) * rows + start, 16), size)
        return pltpu.make_async_remote_copy(
            src_ref=gradient.at[source],
            dst_ref=arrived.at[e, pl.ds(start, size)],
            send_sem=bsend.at[part, d],
            recv_sem=brecv.at[part, d],
            device_id={"expert": e ^ d},
            device_id_type=MESH,
        )

    order = [d for d in range(1, ways) if d & 2] + [d for d in range(1, ways) if not d & 2]

    def started(copies):
        for copy in copies:
            copy.start()
        return copies

    def waited(copies):
        for copy in copies:
            copy.wait()

    indices = started([to_expert(picked, col_picked, isend, irecv, d) for d in order])
    pieces = [started([bulk(d, 0) for d in order])]
    col_picked[e] = picked[e]
    constants[0].wait()

    zero = jnp.zeros((1, LANES), F32)

    def values(out, block_of, where, fetch, begin, end):
        @pl.loop(begin, end)
        def _(s):
            fetch(s).wait()
            found = [
                values_of(block_of(s, j), where[s, j : j + 1, :], turned[...], owner)
                for j in range(units)
            ]
            out[s] = jnp.concatenate(found + [zero] * (8 - units), axis=0)

    def halves(ref, j):
        return [slice(j * 128 + h * SPAN, j * 128 + (h + 1) * SPAN) for h in range(2)]

    def of_momentum(s, j):
        return jnp.concatenate([mn[here, columns(s)] for here in halves(mn, j)], axis=1)

    def of_gradient(s, j):
        return jnp.concatenate([gbuf[s, here, :] for here in halves(gbuf, j)], axis=1)

    values(row_value, of_momentum, picked, fetch_m, 0, ways)
    rows_out = started([to_expert(row_value, row_in, rsend, rrecv, d) for d in order])
    row_in[e] = row_value[e]

    waited(indices)
    mine = pl.ds(pl.multiple_of(r * tiles, 8), tiles)
    all_picked[mine, :] = col_picked[...].reshape(tiles, LANES)
    picked_out = started([to_replica(all_picked, r, asend, arecv, 4, 0)])
    pieces.append(started([bulk(d, 1) for d in order]))

    values(col_value, of_gradient, col_picked, fetch_g, 0, ways)
    cols_out = started([to_expert(col_value, col_in, csend, crecv, d) for d in order])
    col_in[e] = col_value[e]

    waited(rows_out)
    all_value[mine, :] = (DECAY * row_in[...] + col_value[...]).reshape(tiles, LANES)
    value_out = started([to_replica(all_value, r, psend, precv, 4, 0)])
    waited(picked_out)
    picked_out = []
    for n, d in enumerate((1, 2, 3)):
        for h in range(2):
            picked_out.append(to_replica(all_picked, r ^ (4 * h), asend, arecv, d, 1 + 2 * n + h))
    started(picked_out)
    pieces.append(started([bulk(d, 2) for d in order]))
    arrived[e] = gbuf[e]

    waited(cols_out)
    waited(value_out)
    value_out = []
    for n, d in enumerate((1, 2, 3)):
        for h in range(2):
            value_out.append(to_replica(all_value, r ^ (4 * h), psend, precv, d, 1 + 2 * n + h))
    started(value_out)

    @pl.loop(0, ways)
    def _(s):
        value = DECAY * row_value[s] + col_in[s]
        for j in range(units):
            restored = restored_of(
                picked[s, j : j + 1, :], value[j : j + 1, :], turned[...], owner
            )
            for h, here in enumerate(halves(mn, j)):
                mn[here, columns(s)] = (
                    DECAY * mn[here, columns(s)] - restored[:, h * LANES : (h + 1) * LANES]
                )

    constants[1].wait()
    waited(picked_out)
    waited(value_out)
    at = lax.broadcasted_iota(jnp.int32, (SPAN, 256), 0)

    @pl.loop(0, ways)
    def _(s):
        for j in range(units):
            each = pl.ds(s * 8 + j, replicas, stride=tiles)
            parts = []
            for index, value in zip(block_rows_of(all_picked[each, :]), block_rows_of(all_value[each, :])):
                w = [columns_of(turned[...], i >> 6) * v for i, v in zip(index, value)]
                v = jnp.concatenate(index, axis=1) & 63
                at_v = jnp.where(at == v, 1.0, 0.0).astype(BF16)
                t = dot_nt(jnp.concatenate(split(jnp.concatenate(w, axis=1)), axis=0), at_v)
                parts.append(t[:SPAN] + t[SPAN:])
            high, low = split(jnp.concatenate(parts, axis=1))
            th[j * SPAN : (j + 1) * SPAN, :] = high
            tl[j * SPAN : (j + 1) * SPAN, :] = low
        out = dot(th[...], four[0]) + (dot(tl[...], four[0]) + dot(th[...], four[1]))
        for j in range(units):
            for h in range(2):
                here = pl.ds(pl.multiple_of(s * rows + j * 128 + h * SPAN, SPAN), SPAN)
                update[here, :] = out[j * SPAN : (j + 1) * SPAN, h * LANES : (h + 1) * LANES]

    for d in [0] + order:
        if d:
            waited([piece[order.index(d)] for piece in pieces])
        source = e ^ d

        @pl.loop(0, units)
        def _(j):
            here = pl.ds(pl.multiple_of(j * 128, 128), 128)
            mn[here, columns(source)] = mn[here, columns(source)] + arrived[source, here, :].astype(F32)


def step(gradient, momentum, picked, turned, four, ways, replicas):
    rows = momentum.shape[0]
    tile = (ways, 8, LANES)
    dma = pltpu.SemaphoreType.DMA
    cuts = CUTS
    hbm = pl.BlockSpec(memory_space=pltpu.HBM)
    return pl.pallas_call(
        functools.partial(step_kernel, ways=ways, replicas=replicas, cuts=cuts),
        in_specs=[hbm, hbm, VMEM, hbm, hbm],
        out_specs=[VMEM, VMEM],
        out_shape=[
            jax.ShapeDtypeStruct(momentum.shape, F32),
            jax.ShapeDtypeStruct(gradient.shape, F32),
        ],
        scratch_shapes=[
            pltpu.VMEM((ways, rows, LANES), BF16),
            pltpu.VMEM((ways, rows, LANES), BF16),
            pltpu.VMEM(turned.shape, F32),
            pltpu.VMEM((4, SPAN, LANES), BF16),
            pltpu.VMEM(four.shape, BF16),
            pltpu.VMEM(tile, jnp.int32),
            *[pltpu.VMEM(tile, F32)] * 4,
            pltpu.VMEM((replicas * ways * 8, LANES), jnp.int32),
            pltpu.VMEM((replicas * ways * 8, LANES), F32),
            *[pltpu.VMEM((rows // 2, 256), BF16)] * 2,
            dma((ways,)),
            dma((ways,)),
            dma((2,)),
            *[dma((ways,))] * 6,
            *[dma((len(cuts) - 1, ways))] * 2,
            *[dma((7,))] * 4,
        ],
        compiler_params=pltpu.CompilerParams(
            collective_id=0, has_side_effects=True, vmem_limit_bytes=40 << 20
        ),
        name="step",
    )(gradient, momentum, picked, turned, four)


def on_device(gradient, momentum, group_index):
    turned, four = (jnp.asarray(t) for t in tables())
    ways = lax.axis_size("expert")
    replicas = lax.axis_size("dp")
    total_rows = gradient.shape[2]
    rows, cols = momentum.shape[2:]
    units = rows // 128
    wide = cols // SPAN // ways

    gradient = gradient.reshape(total_rows, LANES)
    momentum = momentum.reshape(rows, cols)

    own = lax.dynamic_index_in_dim(group_index, lax.axis_index("dp"), 2, keepdims=False)
    own = own.reshape(units, 2, ways, wide, TOPK).transpose(2, 0, 1, 3, 4).reshape(ways, units, LANES)
    own = jnp.pad(own, ((0, 0), (0, 8 - units), (0, 0)))

    momentum_next, update = step(gradient, momentum, own, turned, four, ways, replicas)
    return momentum_next.reshape(1, 1, rows, cols), update.reshape(1, total_rows, LANES)


def solution(mesh):
    return jax.shard_map(
        on_device,
        mesh=mesh,
        in_specs=(
            P("dp", None, None, "expert"),
            P("dp", None, "expert", None),
            P("expert", None, None, None),
        ),
        out_specs=(P("dp", None, "expert", None), P(None, None, "expert")),
        check_vma=False,
    )
```

```python
import functools

import jax
import jax.numpy as jnp
import numpy as np
from jax import lax
from jax.experimental import pallas as pl
from jax.experimental.pallas import tpu as pltpu
from jax.sharding import PartitionSpec as P

SPAN = 64
TOPK = 32
DECAY = 0.999
LANES = 128
CUTS = (0, 128, 256, 896)
PAIR = 2
SPLIT = 14

F32 = jnp.float32
BF16 = jnp.bfloat16
MESH = pl.DeviceIdType.MESH
VMEM = pl.BlockSpec(memory_space=pltpu.VMEM)


def cosine_table():
    u = np.arange(SPAN, dtype=np.float64)[:, None]
    i = np.arange(SPAN, dtype=np.float64)[None, :]
    weight = np.where(u == 0, np.sqrt(1.0 / SPAN), np.sqrt(2.0 / SPAN))
    return weight * np.cos(np.pi * (2.0 * i + 1.0) * u / (2.0 * SPAN))


def two_parts(x):
    high = x.astype(jnp.bfloat16.dtype)
    low = (x - high.astype(np.float64)).astype(jnp.bfloat16.dtype)
    return high, low


def tables():
    c = cosine_table()
    turned = np.zeros((SPAN, LANES), np.float32)
    turned[:, :SPAN] = c.T
    return turned, np.stack(two_parts(np.kron(np.eye(4), c)))


def split(x):
    high = x.astype(BF16)
    return high, (x - high.astype(F32)).astype(BF16)


def dot(a, b):
    return jnp.dot(a, b, preferred_element_type=F32)


def dot_nt(a, b):
    return lax.dot_general(a, b, (((1,), (1,)), ((), ())), preferred_element_type=F32)


def columns_of(table, row):
    where = jnp.broadcast_to(row, table.shape)
    return jnp.take_along_axis(table, where, axis=1, mode="promise_in_bounds")


def spread(part, owner_ref):
    return jnp.concatenate([part * owner_ref[q] for q in range(4)], axis=0)


def right_side(picked, turned, owner_ref):
    high, low = split(columns_of(turned, picked & 63))
    return jnp.concatenate([spread(high, owner_ref), spread(low, owner_ref)], axis=1)


def values_of(x, picked, turned, owner_ref):
    right = right_side(picked, turned, owner_ref)
    if x.dtype == BF16:
        z = dot(x, right)
        z = z[:, :LANES] + z[:, LANES:]
    else:
        z = dot(jnp.concatenate(split(x), axis=0), right)
        z = z[:SPAN, :LANES] + (z[:SPAN, LANES:] + z[SPAN:, :LANES] + z[SPAN:, LANES:])
    return jnp.sum(columns_of(turned, picked >> 6) * z, axis=0, keepdims=True)


def restored_of(picked, value, turned, owner_ref):
    high, low = split(columns_of(turned, picked >> 6) * value)
    left = jnp.concatenate(
        [jnp.concatenate([high, high], axis=1), jnp.concatenate([low, low], axis=1)], axis=0
    )
    r = dot_nt(left, right_side(picked, turned, owner_ref))
    return r[:SPAN] + r[SPAN:]


def block_rows_of(found):
    replica = lax.broadcasted_iota(jnp.int32, (8, LANES), 0)
    group = lax.broadcasted_iota(jnp.int32, (8, LANES), 1) >> 5
    turned = found
    for n in range(1, 4):
        turned = jnp.where((replica & 3) == n, pltpu.roll(found, TOPK * n, 1), turned)
    rows = []
    for b in range(4):
        here = turned if b == 0 else pltpu.roll(turned, LANES - TOPK * b, 1)
        here = jnp.where((replica & 3) == group, here, jnp.zeros_like(here))
        here = here + pltpu.roll(here, 1, 0)
        here = here + pltpu.roll(here, 2, 0)
        rows.append((here[3:4], here[7:8]))
    return rows


def halves(j):
    return [slice(j * 128 + h * SPAN, j * 128 + (h + 1) * SPAN) for h in range(2)]


def sixteen(row):
    return jnp.broadcast_to(row, (16, row.shape[1]))


def decode(first, slabs, units, picked, value, turned, four, out, start, th, tl):
    replicas = 8
    stride = picked.shape[0] // replicas
    at = (4, 16, 256)
    at = lax.broadcasted_iota(jnp.int32, at, 0) * 16 + lax.broadcasted_iota(jnp.int32, at, 1)
    at = at.astype(F32).astype(BF16)
    one, none = jnp.ones(at.shape, BF16), jnp.zeros(at.shape, BF16)
    for n in range(slabs * units):
        each = pl.ds((first + n // units) * 8 + n % units, replicas, stride=stride)
        parts = []
        for index, val in zip(block_rows_of(picked[each, :]), block_rows_of(value[each, :])):
            w = [columns_of(turned[...], i >> 6) * v for i, v in zip(index, val)]
            v = sixteen((jnp.concatenate(index, axis=1) & 63).astype(F32)).astype(BF16)
            at_v = jnp.where(at == v[None], one, none).reshape(SPAN, 256)
            t = dot_nt(jnp.concatenate(split(jnp.concatenate(w, axis=1)), axis=0), at_v)
            parts.append(t[:SPAN] + t[SPAN:])
        high, low = split(jnp.concatenate(parts, axis=1))
        th[n * SPAN : (n + 1) * SPAN, :] = high
        tl[n * SPAN : (n + 1) * SPAN, :] = low
    whole = dot(th[...], four[0]) + (dot(tl[...], four[0]) + dot(th[...], four[1]))
    for n in range(slabs * units):
        for h in range(2):
            here = pl.ds(pl.multiple_of(start + n * 128 + h * SPAN, SPAN), SPAN)
            out[here, :] = whole[n * SPAN : (n + 1) * SPAN, h * LANES : (h + 1) * LANES]


def step_kernel(
    gradient, momentum, picked, turned_hbm, four_hbm,
    mn, update, all_picked, all_value,
    gbuf, arrived, turned, owner, four, col_picked, row_value, row_in, col_value, col_in, th, tl,
    msem, gsem, csem, isend, irecv, rsend, rrecv, csend, crecv, bsend, brecv,
    asend, arecv, psend, precv,
    *, ways, cuts, slabs,
):
    e = lax.axis_index("expert")
    r = lax.axis_index("dp")
    rows = gbuf.shape[1]
    units = rows // 128
    tiles = ways * 8

    barrier = pltpu.get_barrier_semaphore()
    for d in range(1, ways):
        pl.semaphore_signal(barrier, inc=1, device_id={"expert": e ^ d}, device_id_type=MESH)
    near = (1, 2, 3, 4)
    for d in near:
        pl.semaphore_signal(barrier, inc=1, device_id={"dp": r ^ d}, device_id_type=MESH)

    def columns(s):
        return pl.ds(pl.multiple_of(s * LANES, LANES), LANES)

    def fetch_m(s):
        return pltpu.make_async_copy(momentum.at[:, columns(s)], mn.at[:, columns(s)], msem.at[s])

    def fetch_g(s):
        here = pl.ds(pl.multiple_of(s * rows, 128), rows)
        return pltpu.make_async_copy(gradient.at[here], gbuf.at[s], gsem.at[s])

    constants = [
        pltpu.make_async_copy(turned_hbm, turned, csem.at[0]),
        pltpu.make_async_copy(four_hbm, four, csem.at[1]),
    ]
    constants[0].start()

    @pl.loop(0, ways)
    def _(s):
        fetch_m(s).start()

    @pl.loop(0, ways)
    def _(s):
        fetch_g(s).start()

    constants[1].start()
    lanes = lax.broadcasted_iota(jnp.int32, (SPAN, LANES), 1) >> 5
    for q in range(4):
        owner[q] = jnp.where(lanes == q, 1.0, 0.0).astype(BF16)

    pl.semaphore_wait(barrier, ways - 1 + len(near))

    def to_expert(src, dst, send, recv, d):
        return pltpu.make_async_remote_copy(
            src_ref=src.at[e ^ d],
            dst_ref=dst.at[e],
            send_sem=send.at[d],
            recv_sem=recv.at[d],
            device_id={"expert": e ^ d},
            device_id_type=MESH,
        )

    def to_replica(buf, slot, send, recv, d, n):
        here = pl.ds(pl.multiple_of(slot * tiles, 8), tiles)
        return pltpu.make_async_remote_copy(
            src_ref=buf.at[here],
            dst_ref=buf.at[here],
            send_sem=send.at[n],
            recv_sem=recv.at[n],
            device_id={"dp": r ^ d},
            device_id_type=MESH,
        )

    def bulk(d, part):
        start, size = cuts[part], cuts[part + 1] - cuts[part]
        source = pl.ds(pl.multiple_of((e ^ d) * rows + start, 16), size)
        return pltpu.make_async_remote_copy(
            src_ref=gradient.at[source],
            dst_ref=arrived.at[e, pl.ds(start, size)],
            send_sem=bsend.at[part, d],
            recv_sem=brecv.at[part, d],
            device_id={"expert": e ^ d},
            device_id_type=MESH,
        )

    order = [d for d in range(1, ways) if d & 2] + [d for d in range(1, ways) if not d & 2]

    def started(copies):
        for copy in copies:
            copy.start()
        return copies

    def waited(copies):
        for copy in copies:
            copy.wait()

    indices = started([to_expert(picked, col_picked, isend, irecv, d) for d in order])
    pieces = [started([bulk(d, 0) for d in order])]
    col_picked[e] = picked[e]
    constants[0].wait()

    zero = jnp.zeros((1, LANES), F32)

    def values(out, block_of, where, fetch):
        @pl.loop(0, ways // PAIR)
        def _(t):
            for n in range(PAIR):
                fetch(PAIR * t + n).wait()
            for n in range(PAIR):
                s = PAIR * t + n
                found = [
                    values_of(block_of(s, j), where[s, j : j + 1, :], turned[...], owner)
                    for j in range(units)
                ]
                out[s] = jnp.concatenate(found + [zero] * (8 - units), axis=0)

    def of_momentum(s, j):
        blocks = []
        for here in halves(j):
            blocks.append(DECAY * mn[here, columns(s)])
            mn[here, columns(s)] = blocks[-1]
        return jnp.concatenate(blocks, axis=1)

    def of_gradient(s, j):
        return jnp.concatenate([gbuf[s, here, :] for here in halves(j)], axis=1)

    values(row_value, of_momentum, picked, fetch_m)
    rows_out = started([to_expert(row_value, row_in, rsend, rrecv, d) for d in order])
    row_in[e] = row_value[e]

    waited(indices)
    mine = pl.ds(pl.multiple_of(r * tiles, 8), tiles)
    all_picked[mine, :] = col_picked[...].reshape(tiles, LANES)
    picked_out = started([to_replica(all_picked, r, asend, arecv, 4, 0)])
    pieces.append(started([bulk(d, 1) for d in order]))

    values(col_value, of_gradient, col_picked, fetch_g)
    cols_out = started([to_expert(col_value, col_in, csend, crecv, d) for d in order])
    col_in[e] = col_value[e]

    waited(rows_out)
    all_value[mine, :] = (row_in[...] + col_value[...]).reshape(tiles, LANES)
    value_out = started([to_replica(all_value, r, psend, precv, 4, 0)])
    waited(picked_out)
    picked_out = []
    for n, d in enumerate((1, 2, 3)):
        for h in range(2):
            picked_out.append(to_replica(all_picked, r ^ (4 * h), asend, arecv, d, 1 + 2 * n + h))
    started(picked_out)
    pieces.append(started([bulk(d, 2) for d in order]))

    def add_rows(source, s, start, size):
        here = slice(start, start + size)
        mn[here, columns(s)] = mn[here, columns(s)] + source[s, here, :].astype(F32)

    def add_part(part):
        def one(d):
            bulk(d, part).wait()
            add_rows(arrived, e ^ d, cuts[part], cuts[part + 1] - cuts[part])

        @pl.loop(0, ways // 2)
        def _(n):
            one(4 * (n >> 1) + 2 + (n & 1))

        @pl.loop(1, ways // 2)
        def _(n):
            one(4 * (n >> 1) + (n & 1))

    add_rows(gbuf, e, 0, rows)
    add_part(0)
    waited(cols_out)
    waited(value_out)
    value_out = []
    for n, d in enumerate((1, 2, 3)):
        for h in range(2):
            value_out.append(to_replica(all_value, r ^ (4 * h), psend, precv, d, 1 + 2 * n + h))
    started(value_out)

    @pl.loop(0, ways // PAIR)
    def _(t):
        for n in range(PAIR):
            s = PAIR * t + n
            value = row_value[s] + col_in[s]
            for j in range(units):
                restored = restored_of(
                    picked[s, j : j + 1, :], value[j : j + 1, :], turned[...], owner
                )
                for h, here in enumerate(halves(j)):
                    mn[here, columns(s)] = mn[here, columns(s)] - restored[:, h * LANES : (h + 1) * LANES]

    add_part(1)
    constants[1].wait()
    waited(picked_out)
    waited(value_out)

    @pl.loop(0, slabs)
    def _(s):
        decode(s, 1, units, all_picked, all_value, turned, four, update, s * rows, th, tl)

    add_part(2)


def place(array):
    return pltpu.with_memory_space_constraint(array, pltpu.HBM)


def step(gradient, momentum, picked, turned, four, ways, replicas):
    rows = momentum.shape[0]
    tile = (ways, 8, LANES)
    dma = pltpu.SemaphoreType.DMA
    hbm = pl.BlockSpec(memory_space=pltpu.HBM)
    return pl.pallas_call(
        functools.partial(step_kernel, ways=ways, cuts=CUTS, slabs=SPLIT),
        in_specs=[hbm, hbm, VMEM, hbm, hbm],
        out_specs=[VMEM] * 4,
        out_shape=[
            jax.ShapeDtypeStruct(momentum.shape, F32),
            jax.ShapeDtypeStruct((SPLIT * rows, LANES), F32),
            jax.ShapeDtypeStruct((replicas * ways * 8, LANES), jnp.int32),
            jax.ShapeDtypeStruct((replicas * ways * 8, LANES), F32),
        ],
        scratch_shapes=[
            pltpu.VMEM((ways, rows, LANES), BF16),
            pltpu.VMEM((ways, rows, LANES), BF16),
            pltpu.VMEM(turned.shape, F32),
            pltpu.VMEM((4, SPAN, LANES), BF16),
            pltpu.VMEM(four.shape, BF16),
            pltpu.VMEM(tile, jnp.int32),
            *[pltpu.VMEM(tile, F32)] * 4,
            *[pltpu.VMEM((rows // 2, 256), BF16)] * 2,
            dma((ways,)),
            dma((ways,)),
            dma((2,)),
            *[dma((ways,))] * 6,
            *[dma((len(CUTS) - 1, ways))] * 2,
            *[dma((7,))] * 4,
        ],
        compiler_params=pltpu.CompilerParams(
            collective_id=0, has_side_effects=True, vmem_limit_bytes=20 << 20
        ),
        name="step",
    )(gradient, momentum, picked, turned, four)


def finish_kernel(
    mn, update, all_picked, all_value, turned_hbm, four_hbm,
    mn_out, update_out,
    turned, four, tail, th, tl, csem, msem, usem,
    *, ways,
):
    rows = mn.shape[0]
    units = rows // 128
    done = update.shape[0] // rows
    constants = [
        pltpu.make_async_copy(turned_hbm, turned, csem.at[0]),
        pltpu.make_async_copy(four_hbm, four, csem.at[1]),
    ]
    for copy in constants:
        copy.start()

    def slab(s, n=1):
        return pl.ds(s * rows, n * rows)

    copies = [
        pltpu.make_async_copy(update.at[slab(s)], update_out.at[slab(s)], usem.at[s]) for s in range(done)
    ]
    for j in range(units):
        here = pl.ds(j * 128, 128)
        copies.append(pltpu.make_async_copy(mn.at[here], mn_out.at[here], msem.at[j]))
    for copy in copies:
        copy.start()
    for copy in constants:
        copy.wait()

    @pl.loop(done, ways)
    def _(s):
        decode(s, 1, units, all_picked, all_value, turned, four, tail, (s - done) * rows, th, tl)

    for s in range(done, ways):
        copies.append(pltpu.make_async_copy(tail.at[slab(s - done)], update_out.at[slab(s)], usem.at[s]))
        copies[-1].start()
    for copy in copies:
        copy.wait()


def finish(mn, update, all_picked, all_value, turned, four, ways):
    rows = mn.shape[0]
    dma = pltpu.SemaphoreType.DMA
    hbm = pl.BlockSpec(memory_space=pltpu.HBM)
    return pl.pallas_call(
        functools.partial(finish_kernel, ways=ways),
        in_specs=[VMEM] * 4 + [hbm] * 2,
        out_specs=[hbm] * 2,
        out_shape=[
            jax.ShapeDtypeStruct(mn.shape, F32),
            jax.ShapeDtypeStruct((ways * rows, LANES), F32),
        ],
        scratch_shapes=[
            pltpu.VMEM(turned.shape, F32),
            pltpu.VMEM(four.shape, BF16),
            pltpu.VMEM(((ways - SPLIT) * rows, LANES), F32),
            *[pltpu.VMEM((rows // 2, 256), BF16)] * 2,
            dma((2,)),
            dma((rows // 128,)),
            dma((ways,)),
        ],
        compiler_params=pltpu.CompilerParams(vmem_limit_bytes=12 << 20),
        name="finish",
    )(mn, update, all_picked, all_value, turned, four)


def on_device(gradient, momentum, group_index):
    turned, four = (place(jnp.asarray(t)) for t in tables())
    ways = lax.axis_size("expert")
    replicas = lax.axis_size("dp")
    total_rows = gradient.shape[2]
    rows, cols = momentum.shape[2:]
    units = rows // 128
    wide = cols // SPAN // ways

    gradient = place(gradient.reshape(total_rows, LANES))
    momentum = place(momentum.reshape(rows, cols))

    own = lax.dynamic_index_in_dim(group_index, lax.axis_index("dp"), 2, keepdims=False)
    own = own.reshape(units, 2, ways, wide, TOPK).transpose(2, 0, 1, 3, 4).reshape(ways, units, LANES)
    own = jnp.pad(own, ((0, 0), (0, 8 - units), (0, 0)))

    parts = step(gradient, momentum, own, turned, four, ways, replicas)
    momentum_next, update = finish(*parts, turned, four, ways)
    return momentum_next.reshape(1, 1, rows, cols), update.reshape(1, total_rows, LANES)


def solution(mesh):
    return jax.shard_map(
        on_device,
        mesh=mesh,
        in_specs=(
            P("dp", None, None, "expert"),
            P("dp", None, "expert", None),
            P("expert", None, None, None),
        ),
        out_specs=(P("dp", None, "expert", None), P(None, None, "expert")),
        check_vma=False,
    )
```

```python
import functools

import jax
import jax.numpy as jnp
import numpy as np
from jax import lax
from jax.experimental import pallas as pl
from jax.experimental.pallas import tpu as pltpu
from jax.sharding import PartitionSpec as P

SPAN = 64
TOPK = 32
DECAY = 0.999
LANES = 128
CUTS = (0, 128, 256, 896)
PAIR = 2
SPLIT = 14

F32 = jnp.float32
BF16 = jnp.bfloat16
MESH = pl.DeviceIdType.MESH
VMEM = pl.BlockSpec(memory_space=pltpu.VMEM)


def cosine_table():
    u = np.arange(SPAN, dtype=np.float64)[:, None]
    i = np.arange(SPAN, dtype=np.float64)[None, :]
    weight = np.where(u == 0, np.sqrt(1.0 / SPAN), np.sqrt(2.0 / SPAN))
    return weight * np.cos(np.pi * (2.0 * i + 1.0) * u / (2.0 * SPAN))


def two_parts(x):
    high = x.astype(jnp.bfloat16.dtype)
    low = (x - high.astype(np.float64)).astype(jnp.bfloat16.dtype)
    return high, low


def tables():
    c = cosine_table()
    turned = np.zeros((SPAN, LANES), np.float32)
    turned[:, :SPAN] = c.T
    return turned, np.stack(two_parts(np.kron(np.eye(4), c)))


def split(x):
    high = x.astype(BF16)
    return high, (x - high.astype(F32)).astype(BF16)


def dot(a, b):
    return jnp.dot(a, b, preferred_element_type=F32)


def dot_nt(a, b):
    return lax.dot_general(a, b, (((1,), (1,)), ((), ())), preferred_element_type=F32)


def columns_of(table, row):
    where = jnp.broadcast_to(row, table.shape)
    return jnp.take_along_axis(table, where, axis=1, mode="promise_in_bounds")


def spread(part, owner_ref):
    return jnp.concatenate([part * owner_ref[q] for q in range(4)], axis=0)


def right_side(picked, turned, owner_ref):
    high, low = split(columns_of(turned, picked & 63))
    return jnp.concatenate([spread(high, owner_ref), spread(low, owner_ref)], axis=1)


def values_of(x, picked, turned, owner_ref):
    right = right_side(picked, turned, owner_ref)
    if x.dtype == BF16:
        z = dot(x, right)
        z = z[:, :LANES] + z[:, LANES:]
    else:
        z = dot(jnp.concatenate(split(x), axis=0), right)
        z = z[:SPAN, :LANES] + (z[:SPAN, LANES:] + z[SPAN:, :LANES] + z[SPAN:, LANES:])
    return jnp.sum(columns_of(turned, picked >> 6) * z, axis=0, keepdims=True)


def restored_of(picked, value, turned, owner_ref):
    high, low = split(columns_of(turned, picked >> 6) * value)
    left = jnp.concatenate(
        [jnp.concatenate([high, high], axis=1), jnp.concatenate([low, low], axis=1)], axis=0
    )
    r = dot_nt(left, right_side(picked, turned, owner_ref))
    return r[:SPAN] + r[SPAN:]


def block_rows_of(found):
    replica = lax.broadcasted_iota(jnp.int32, (8, LANES), 0)
    group = lax.broadcasted_iota(jnp.int32, (8, LANES), 1) >> 5
    turned = found
    for n in range(1, 4):
        turned = jnp.where((replica & 3) == n, pltpu.roll(found, TOPK * n, 1), turned)
    rows = []
    for b in range(4):
        here = turned if b == 0 else pltpu.roll(turned, LANES - TOPK * b, 1)
        here = jnp.where((replica & 3) == group, here, jnp.zeros_like(here))
        here = here + pltpu.roll(here, 1, 0)
        here = here + pltpu.roll(here, 2, 0)
        rows.append((here[3:4], here[7:8]))
    return rows


def halves(j):
    return [slice(j * 128 + h * SPAN, j * 128 + (h + 1) * SPAN) for h in range(2)]


def sixteen(row):
    return jnp.broadcast_to(row, (16, row.shape[1]))


def decode(first, slabs, units, picked, value, turned, four, out, start, th, tl):
    replicas = 8
    stride = picked.shape[0] // replicas
    at = (4, 16, 256)
    at = lax.broadcasted_iota(jnp.int32, at, 0) * 16 + lax.broadcasted_iota(jnp.int32, at, 1)
    at = at.astype(F32).astype(BF16)
    one, none = jnp.ones(at.shape, BF16), jnp.zeros(at.shape, BF16)
    for n in range(slabs * units):
        each = pl.ds((first + n // units) * 8 + n % units, replicas, stride=stride)
        parts = []
        for index, val in zip(block_rows_of(picked[each, :]), block_rows_of(value[each, :])):
            w = [columns_of(turned[...], i >> 6) * v for i, v in zip(index, val)]
            v = sixteen((jnp.concatenate(index, axis=1) & 63).astype(F32)).astype(BF16)
            at_v = jnp.where(at == v[None], one, none).reshape(SPAN, 256)
            t = dot_nt(jnp.concatenate(split(jnp.concatenate(w, axis=1)), axis=0), at_v)
            parts.append(t[:SPAN] + t[SPAN:])
        high, low = split(jnp.concatenate(parts, axis=1))
        th[n * SPAN : (n + 1) * SPAN, :] = high
        tl[n * SPAN : (n + 1) * SPAN, :] = low
    whole = dot(th[...], four[0]) + (dot(tl[...], four[0]) + dot(th[...], four[1]))
    for n in range(slabs * units):
        for h in range(2):
            here = pl.ds(pl.multiple_of(start + n * 128 + h * SPAN, SPAN), SPAN)
            out[here, :] = whole[n * SPAN : (n + 1) * SPAN, h * LANES : (h + 1) * LANES]


def step_kernel(
    gradient, momentum, picked, turned_hbm, four_hbm,
    mn, update, all_picked, all_value,
    gbuf, arrived, turned, owner, four, col_picked, row_value, row_in, col_value, col_in, th, tl,
    msem, gsem, csem, isend, irecv, rsend, rrecv, csend, crecv, bsend, brecv,
    asend, arecv, psend, precv,
    *, ways, cuts, slabs,
):
    e = lax.axis_index("expert")
    r = lax.axis_index("dp")
    rows = gbuf.shape[1]
    units = rows // 128
    tiles = ways * 8

    barrier = pltpu.get_barrier_semaphore()
    for d in range(1, ways):
        pl.semaphore_signal(barrier, inc=1, device_id={"expert": e ^ d}, device_id_type=MESH)
    near = (1, 2, 3, 4)
    for d in near:
        pl.semaphore_signal(barrier, inc=1, device_id={"dp": r ^ d}, device_id_type=MESH)

    def columns(s):
        return pl.ds(pl.multiple_of(s * LANES, LANES), LANES)

    def fetch_m(s):
        return pltpu.make_async_copy(momentum.at[:, columns(s)], mn.at[:, columns(s)], msem.at[s])

    def fetch_g(s):
        here = pl.ds(pl.multiple_of(s * rows, 128), rows)
        return pltpu.make_async_copy(gradient.at[here], gbuf.at[s], gsem.at[s])

    constants = [
        pltpu.make_async_copy(turned_hbm, turned, csem.at[0]),
        pltpu.make_async_copy(four_hbm, four, csem.at[1]),
    ]
    constants[0].start()

    @pl.loop(0, ways)
    def _(s):
        fetch_m(s).start()

    @pl.loop(0, ways)
    def _(s):
        fetch_g(s).start()

    constants[1].start()
    lanes = lax.broadcasted_iota(jnp.int32, (SPAN, LANES), 1) >> 5
    for q in range(4):
        owner[q] = jnp.where(lanes == q, 1.0, 0.0).astype(BF16)

    pl.semaphore_wait(barrier, ways - 1 + len(near))

    def to_expert(src, dst, send, recv, d):
        return pltpu.make_async_remote_copy(
            src_ref=src.at[e ^ d],
            dst_ref=dst.at[e],
            send_sem=send.at[d],
            recv_sem=recv.at[d],
            device_id={"expert": e ^ d},
            device_id_type=MESH,
        )

    def to_replica(buf, slot, send, recv, d, n):
        here = pl.ds(pl.multiple_of(slot * tiles, 8), tiles)
        return pltpu.make_async_remote_copy(
            src_ref=buf.at[here],
            dst_ref=buf.at[here],
            send_sem=send.at[n],
            recv_sem=recv.at[n],
            device_id={"dp": r ^ d},
            device_id_type=MESH,
        )

    def bulk(d, part):
        start, size = cuts[part], cuts[part + 1] - cuts[part]
        source = pl.ds(pl.multiple_of((e ^ d) * rows + start, 16), size)
        return pltpu.make_async_remote_copy(
            src_ref=gradient.at[source],
            dst_ref=arrived.at[e, pl.ds(start, size)],
            send_sem=bsend.at[part, d],
            recv_sem=brecv.at[part, d],
            device_id={"expert": e ^ d},
            device_id_type=MESH,
        )

    order = [d for d in range(1, ways) if d & 2] + [d for d in range(1, ways) if not d & 2]

    def started(copies):
        for copy in copies:
            copy.start()
        return copies

    def waited(copies):
        for copy in copies:
            copy.wait()

    indices = started([to_expert(picked, col_picked, isend, irecv, d) for d in order])
    pieces = [started([bulk(d, 0) for d in order])]
    col_picked[e] = picked[e]
    constants[0].wait()

    zero = jnp.zeros((1, LANES), F32)

    def values(out, block_of, where, fetch):
        @pl.loop(0, ways // PAIR)
        def _(t):
            for n in range(PAIR):
                fetch(PAIR * t + n).wait()
            for n in range(PAIR):
                s = PAIR * t + n
                found = [
                    values_of(block_of(s, j), where[s, j : j + 1, :], turned[...], owner)
                    for j in range(units)
                ]
                out[s] = jnp.concatenate(found + [zero] * (8 - units), axis=0)

    def of_momentum(s, j):
        blocks = []
        for here in halves(j):
            blocks.append(DECAY * mn[here, columns(s)])
            mn[here, columns(s)] = blocks[-1]
        return jnp.concatenate(blocks, axis=1)

    def of_gradient(s, j):
        return jnp.concatenate([gbuf[s, here, :] for here in halves(j)], axis=1)

    values(row_value, of_momentum, picked, fetch_m)
    rows_out = started([to_expert(row_value, row_in, rsend, rrecv, d) for d in order])
    row_in[e] = row_value[e]

    waited(indices)
    mine = pl.ds(pl.multiple_of(r * tiles, 8), tiles)
    all_picked[mine, :] = col_picked[...].reshape(tiles, LANES)
    picked_out = started([to_replica(all_picked, r, asend, arecv, d, n) for n, d in enumerate((4, 1, 2, 3))])
    pieces.append(started([bulk(d, 1) for d in order]))

    values(col_value, of_gradient, col_picked, fetch_g)
    cols_out = started([to_expert(col_value, col_in, csend, crecv, d) for d in order])
    col_in[e] = col_value[e]

    waited(rows_out)
    all_value[mine, :] = (row_in[...] + col_value[...]).reshape(tiles, LANES)
    value_out = started([to_replica(all_value, r, psend, precv, d, n) for n, d in enumerate((4, 1, 2, 3))])
    waited(picked_out[:1])
    passed = [to_replica(all_picked, r ^ 4, asend, arecv, d, 3 + d) for d in (1, 2, 3)]
    picked_out = picked_out[1:] + started(passed)
    pieces.append(started([bulk(d, 2) for d in order]))

    def add_rows(source, s, start, size):
        here = slice(start, start + size)
        mn[here, columns(s)] = mn[here, columns(s)] + source[s, here, :].astype(F32)

    def add_part(part):
        def one(d):
            bulk(d, part).wait()
            add_rows(arrived, e ^ d, cuts[part], cuts[part + 1] - cuts[part])

        @pl.loop(0, ways // 2)
        def _(n):
            one(4 * (n >> 1) + 2 + (n & 1))

        @pl.loop(1, ways // 2)
        def _(n):
            one(4 * (n >> 1) + (n & 1))

    add_rows(gbuf, e, 0, rows)
    add_part(0)
    waited(value_out[:1])
    passed = [to_replica(all_value, r ^ 4, psend, precv, d, 3 + d) for d in (1, 2, 3)]
    value_out = value_out[1:] + started(passed)
    waited(cols_out)

    @pl.loop(0, ways // PAIR)
    def _(t):
        for n in range(PAIR):
            s = PAIR * t + n
            value = row_value[s] + col_in[s]
            for j in range(units):
                restored = restored_of(
                    picked[s, j : j + 1, :], value[j : j + 1, :], turned[...], owner
                )
                for h, here in enumerate(halves(j)):
                    mn[here, columns(s)] = mn[here, columns(s)] - restored[:, h * LANES : (h + 1) * LANES]

    add_part(1)
    constants[1].wait()
    waited(picked_out)
    waited(value_out)

    @pl.loop(0, slabs)
    def _(s):
        decode(s, 1, units, all_picked, all_value, turned, four, update, s * rows, th, tl)

    add_part(2)


def place(array):
    return pltpu.with_memory_space_constraint(array, pltpu.HBM)


def step(gradient, momentum, picked, turned, four, ways, replicas):
    rows = momentum.shape[0]
    tile = (ways, 8, LANES)
    dma = pltpu.SemaphoreType.DMA
    hbm = pl.BlockSpec(memory_space=pltpu.HBM)
    return pl.pallas_call(
        functools.partial(step_kernel, ways=ways, cuts=CUTS, slabs=SPLIT),
        in_specs=[hbm, hbm, VMEM, hbm, hbm],
        out_specs=[VMEM] * 4,
        out_shape=[
            jax.ShapeDtypeStruct(momentum.shape, F32),
            jax.ShapeDtypeStruct((SPLIT * rows, LANES), F32),
            jax.ShapeDtypeStruct((replicas * ways * 8, LANES), jnp.int32),
            jax.ShapeDtypeStruct((replicas * ways * 8, LANES), F32),
        ],
        scratch_shapes=[
            pltpu.VMEM((ways, rows, LANES), BF16),
            pltpu.VMEM((ways, rows, LANES), BF16),
            pltpu.VMEM(turned.shape, F32),
            pltpu.VMEM((4, SPAN, LANES), BF16),
            pltpu.VMEM(four.shape, BF16),
            pltpu.VMEM(tile, jnp.int32),
            *[pltpu.VMEM(tile, F32)] * 4,
            *[pltpu.VMEM((rows // 2, 256), BF16)] * 2,
            dma((ways,)),
            dma((ways,)),
            dma((2,)),
            *[dma((ways,))] * 6,
            *[dma((len(CUTS) - 1, ways))] * 2,
            *[dma((7,))] * 4,
        ],
        compiler_params=pltpu.CompilerParams(
            collective_id=0, has_side_effects=True, vmem_limit_bytes=20 << 20
        ),
        name="step",
    )(gradient, momentum, picked, turned, four)


def finish_kernel(
    mn, update, all_picked, all_value, turned_hbm, four_hbm,
    mn_out, update_out,
    turned, four, tail, th, tl, csem, msem, usem,
    *, ways,
):
    rows = mn.shape[0]
    units = rows // 128
    done = update.shape[0] // rows
    constants = [
        pltpu.make_async_copy(turned_hbm, turned, csem.at[0]),
        pltpu.make_async_copy(four_hbm, four, csem.at[1]),
    ]
    for copy in constants:
        copy.start()

    def slab(s, n=1):
        return pl.ds(s * rows, n * rows)

    copies = [
        pltpu.make_async_copy(update.at[slab(s)], update_out.at[slab(s)], usem.at[s]) for s in range(done)
    ]
    for j in range(units):
        here = pl.ds(j * 128, 128)
        copies.append(pltpu.make_async_copy(mn.at[here], mn_out.at[here], msem.at[j]))
    for copy in copies:
        copy.start()
    for copy in constants:
        copy.wait()

    @pl.loop(done, ways)
    def _(s):
        decode(s, 1, units, all_picked, all_value, turned, four, tail, (s - done) * rows, th, tl)

    for s in range(done, ways):
        copies.append(pltpu.make_async_copy(tail.at[slab(s - done)], update_out.at[slab(s)], usem.at[s]))
        copies[-1].start()
    for copy in copies:
        copy.wait()


def finish(mn, update, all_picked, all_value, turned, four, ways):
    rows = mn.shape[0]
    dma = pltpu.SemaphoreType.DMA
    hbm = pl.BlockSpec(memory_space=pltpu.HBM)
    return pl.pallas_call(
        functools.partial(finish_kernel, ways=ways),
        in_specs=[VMEM] * 4 + [hbm] * 2,
        out_specs=[hbm] * 2,
        out_shape=[
            jax.ShapeDtypeStruct(mn.shape, F32),
            jax.ShapeDtypeStruct((ways * rows, LANES), F32),
        ],
        scratch_shapes=[
            pltpu.VMEM(turned.shape, F32),
            pltpu.VMEM(four.shape, BF16),
            pltpu.VMEM(((ways - SPLIT) * rows, LANES), F32),
            *[pltpu.VMEM((rows // 2, 256), BF16)] * 2,
            dma((2,)),
            dma((rows // 128,)),
            dma((ways,)),
        ],
        compiler_params=pltpu.CompilerParams(vmem_limit_bytes=12 << 20),
        name="finish",
    )(mn, update, all_picked, all_value, turned, four)


def on_device(gradient, momentum, group_index):
    turned, four = (place(jnp.asarray(t)) for t in tables())
    ways = lax.axis_size("expert")
    replicas = lax.axis_size("dp")
    total_rows = gradient.shape[2]
    rows, cols = momentum.shape[2:]
    units = rows // 128
    wide = cols // SPAN // ways

    gradient = place(gradient.reshape(total_rows, LANES))
    momentum = place(momentum.reshape(rows, cols))

    own = lax.dynamic_index_in_dim(group_index, lax.axis_index("dp"), 2, keepdims=False)
    own = own.reshape(units, 2, ways, wide, TOPK).transpose(2, 0, 1, 3, 4).reshape(ways, units, LANES)
    own = jnp.pad(own, ((0, 0), (0, 8 - units), (0, 0)))

    parts = step(gradient, momentum, own, turned, four, ways, replicas)
    momentum_next, update = finish(*parts, turned, four, ways)
    return momentum_next.reshape(1, 1, rows, cols), update.reshape(1, total_rows, LANES)


def solution(mesh):
    return jax.shard_map(
        on_device,
        mesh=mesh,
        in_specs=(
            P("dp", None, None, "expert"),
            P("dp", None, "expert", None),
            P("expert", None, None, None),
        ),
        out_specs=(P("dp", None, "expert", None), P(None, None, "expert")),
        check_vma=False,
    )
```
